32 devices in a mesh: ep: 4 (over y, core), fsdp: 8 (over z, x).
Axes of the slice: x: 2, y: 2, z: 4, core: 2. Of those that a mesh axis runs over, the one named last changes fastest.
Arguments:
- master_down: float32 [16, 6400, 4096], P('ep', None, 'fsdp'), may hold values from -0.109375 to 0.109375
- second_down: bfloat16 [16, 6400, 4096], P('ep', None, 'fsdp'), may hold values from -0.0390625 to 0.0390625
- router_weight: float32 [4096, 16], P('fsdp', 'ep'), may hold values from -0.09375 to 0.09375
- router_gain: float32 [4096], P('fsdp'), may hold values from 0.25 to 1.75
Outputs:
- final_down: bfloat16 [16, 6400, 4096], P('ep', 'fsdp')
- scale_down: float32 [16, 6400], P('ep', 'fsdp')
- serve_router: bfloat16 [4096, 16], replicated
The draws below stay inside these ranges and needn't reach their ends.
All inputs are finite; a program needn't handle non-finite values.
Results may differ from the reference program's by a relative error of at most 0.001.
Values may be sent and summed in bfloat16 or wider, within the bound.
A program may use at most 256 MiB of HBM per device.

```python
import jax
import jax.numpy as jnp
from jax import lax

EXPERTS = 16
D_MODEL = 4096
D_EXPERT = 6400


def raised(result, own_key, source, target, shards_of, factor):
    owner, partner = [(jnp.arange(result.shape[dim]) // (result.shape[dim] // shards_of)).reshape([-1 if axis == dim else 1 for axis in range(result.ndim)]) for dim in (source, target)]
    chosen = jax.random.permutation(own_key, shards_of)[partner]
    strong = (owner == chosen) | (owner == (partner + shards_of // 2) % shards_of)
    return jnp.where(strong, factor * result, result)


def steps_of(own_key, shape, shards, smallest, top_value):
    factor_of, own = 1.0, jax.random.fold_in(own_key, 6)
    for position, blocks in shards:
        draws = jnp.exp(jax.random.uniform(jax.random.fold_in(own, position), (blocks,), jnp.float32, smallest / len(shards), top_value / len(shards)))
        factor_of = factor_of * jnp.repeat(draws, shape[position] // blocks).reshape([-1 if axis == position else 1 for axis in range(len(shape))])
    return factor_of


def noise(rng, dims, width, limit, cuts=(), kind=jnp.bfloat16):
    drawn = width * jax.random.normal(rng, dims, jnp.float32)
    if cuts:
        drawn = drawn * steps_of(rng, dims, cuts, -0.22, 0.18)
    return jnp.clip(drawn, -limit, limit).astype(kind)


def heavy_noise(stream_key, dims, width, limit, cuts, heavy, kind=jnp.bfloat16):
    entries = width * jax.random.normal(stream_key, dims, jnp.float32)
    if cuts:
        entries = entries * steps_of(stream_key, dims, cuts, -0.22, 0.18)
    return jnp.clip(raised(entries, jax.random.fold_in(stream_key, 3), *heavy), -limit, limit).astype(kind)


def setup_inputs(seed: int = 0) -> dict:
    arg_keys = jax.random.split(jax.random.key(seed), 5)
    return {
        "master_down": heavy_noise(arg_keys[0], (EXPERTS, D_EXPERT, D_MODEL), D_EXPERT ** -0.5, 0.109375, ((0, 4), (2, 8)), (2, 1, 8, 2.0), jnp.float32),
        "second_down": noise(arg_keys[1], (EXPERTS, D_EXPERT, D_MODEL), (D_EXPERT * 4) ** -0.5, 0.0390625, ((0, 4), (2, 8))),
        "router_weight": noise(arg_keys[2], (D_MODEL, EXPERTS), D_MODEL ** -0.5, 0.09375, ((0, 8), (1, 4)), jnp.float32),
        "router_gain": jnp.clip(1.0 + 0.15 * jax.random.normal(arg_keys[3], (D_MODEL,), jnp.float32), 0.25, 1.75),
    }


def reference(master_down, second_down, router_weight, router_gain):
    merged_down = master_down + second_down.astype(jnp.float32)
    scale_down = jnp.sqrt(lax.optimization_barrier(jnp.sum(merged_down * merged_down, axis=2)))
    final_down = (merged_down / jnp.expand_dims(scale_down, 2)).astype(jnp.bfloat16)
    serve_router = (router_weight * router_gain[:, None]).astype(jnp.bfloat16)
    return (final_down, scale_down, serve_router)
```

```python
import functools

import jax
import jax.numpy as jnp
from jax import lax
from jax.experimental import pallas as pl
from jax.experimental.pallas import tpu as pltpu
from jax.sharding import PartitionSpec as P

MESH = pl.DeviceIdType.MESH
LANES = 128
AHEAD = 2
SLOTS = 4
FETCH = 3


def largest_divisor(size, limit, step):
    return max(d for d in range(step, limit + 1, step) if size % d == 0)


def exchange(dims, master, second, router, gain, final, scales, routers,
             held, narrow, part, whole, gathered, cross, inverse, sent, router_in, gain_in, router_part,
             master_sem, second_sem, small_sem, whole_send, whole_recv, near_send, near_recv, far_send, far_recv,
             back_send, back_recv, block_send, block_recv, router_send, router_recv):
    groups, fsdp, experts, steps, rows, width, first, ring, wide = dims
    chunks, half = experts * steps, fsdp // 2
    me, group = lax.axis_index("fsdp"), lax.axis_index("ep")
    side, lane = me // half, lax.rem(me, half)
    peers = [lax.rem(me + k, fsdp) for k in range(1, fsdp)]
    near = [lax.rem(lane + k, half) for k in range(1, half)]
    others = [lax.rem(group + k, groups) for k in range(1, groups)]
    partner = lax.rem(me + half, fsdp)

    def load(t):
        e, s = t // steps, lax.rem(t, steps)
        span = pl.ds(pl.multiple_of(s * rows, 8), rows)
        a, b = lax.rem(t, ring), lax.rem(t, wide)
        return (
            pltpu.make_async_copy(master.at[e, :, span, :], held.at[a], master_sem.at[a]),
            pltpu.make_async_copy(second.at[e, :, span, :], narrow.at[b], second_sem.at[b]),
        )

    for t in range(min(FETCH, chunks)):
        for copy in load(t):
            copy.start()
    small = (pltpu.make_async_copy(router, router_in, small_sem.at[0]),
             pltpu.make_async_copy(gain, gain_in, small_sem.at[1]))
    for copy in small:
        copy.start()

    barrier = pltpu.get_barrier_semaphore()
    for p in peers:
        pl.semaphore_signal(barrier, inc=1, device_id={"fsdp": p}, device_id_type=MESH)
    for g in others:
        pl.semaphore_signal(barrier, inc=1, device_id={"ep": g}, device_id_type=MESH)

    def remote(source, target, send, recv, p):
        return pltpu.make_async_remote_copy(
            source, target, send, recv, device_id={"fsdp": p}, device_id_type=MESH)

    def sums(t):
        for copy in load(t):
            copy.wait()
        a, b = lax.rem(t, ring), lax.rem(t, wide)

        def body(j, _):
            for s in range(2):
                d = s * half + j
                x = held[a, d] + narrow[b, d].astype(jnp.float32)
                held[a, d] = x
                x = x * x
                acc = x[:, :LANES]
                for c in range(LANES, width, LANES):
                    acc = acc + x[:, c:c + LANES]
                if rows < LANES:
                    acc = jnp.concatenate([acc, jnp.zeros((LANES - rows, LANES), jnp.float32)], axis=0)
                part[t, j, pl.ds(s, 1), :] = jnp.sum(acc.T, axis=0, keepdims=True)
            return 0

        lax.fori_loop(0, half, body, 0)

        @pl.when(t + FETCH < chunks)
        def _():
            for copy in load(t + FETCH):
                copy.start()

    def send_whole(t):
        whole[t, me] = part[t]
        for p in peers:
            remote(part.at[t], whole.at[t, me], whole_send.at[t], whole_recv.at[t], p).start()

    def send_near(t):
        gathered[t, lane] = part[t, lane]
        for q in near:
            remote(part.at[t, q], gathered.at[t, lane], near_send.at[t], near_recv.at[t], side * half + q).start()

    def many(ref, t, count, sem):
        block = ref.at[t, pl.ds(0, count)]
        return pltpu.make_async_copy(block, block, sem)

    def put_scale(t, scale):
        scales[t] = jnp.where(side == 0, scale[0:1], scale[1:2])

    def send_far(t):
        many(gathered, t, half - 1, near_recv.at[t]).wait()
        cross[t, side] = jnp.sum(gathered[t], axis=0)
        remote(cross.at[t, side], cross.at[t, side], far_send.at[t], far_recv.at[t], partner).start()

    def send_back(t):
        many(cross, t, 1, far_recv.at[t]).wait()
        scale = jnp.sqrt(cross[t, 0] + cross[t, 1])
        put_scale(t, scale)
        inverse[t, lane] = 1.0 / scale
        for q in near:
            remote(inverse.at[t, lane], inverse.at[t, lane], back_send.at[t], back_recv.at[t], side * half + q).start()

    def take_whole(t):
        many(whole, t, fsdp - 1, whole_recv.at[t]).wait()
        total = whole[t, 0]
        for k in range(1, fsdp):
            total = total + whole[t, k]
        scale = jnp.sqrt(total)
        inverse[t] = 1.0 / scale
        gathered[0] = scale
        put_scale(t, gathered[0, lane])
        many(whole, t, fsdp - 1, whole_send.at[t]).wait()

    def take_back(t):
        many(inverse, t, half - 1, back_recv.at[t]).wait()
        many(gathered, t, half - 1, near_send.at[t]).wait()
        many(cross, t, 1, far_send.at[t]).wait()
        many(inverse, t, half - 1, back_send.at[t]).wait()

    def drain(t):
        many(sent, lax.rem(t, SLOTS), fsdp - 1, block_send.at[lax.rem(t, SLOTS)]).wait()

    def norm(t):
        @pl.when(t >= SLOTS)
        def _():
            drain(t - SLOTS)

        e, s = t // steps, lax.rem(t, steps)
        a, out = lax.rem(t, ring), lax.rem(t, SLOTS)
        span = pl.ds(pl.multiple_of(s * rows, 8), rows)
        place = final.at[e, span, pl.ds(pl.multiple_of(me * width, LANES), width)]

        def block(d):
            row = inverse[t, lax.rem(d, half), pl.ds(d // half, 1), :]
            factor = jnp.broadcast_to(row, (LANES, LANES)).T[:rows]
            for c in range(0, width, LANES):
                sent[out, d, :, c:c + LANES] = (held[a, d, :, c:c + LANES] * factor).astype(jnp.bfloat16)

        def push(d):
            remote(sent.at[out, d], place, block_send.at[out], block_recv.at[me], d).start()

        def body(k, _):
            block(lax.rem(me + k, fsdp))

            @pl.when(k > 1)
            def _():
                push(lax.rem(me + k - 1, fsdp))

            return 0

        lax.fori_loop(1, fsdp, body, 0)
        block(me)
        push(lax.rem(me + fsdp - 1, fsdp))
        final[e, span, pl.ds(pl.multiple_of(me * width, LANES), width)] = sent[out, me]

    sums(0)
    pl.semaphore_wait(barrier, len(peers) + len(others))

    def start(t, _):
        @pl.when(t > 0)
        def _():
            sums(t)

        send_whole(t)
        return 0

    lax.fori_loop(0, first, start, 0)

    def step(u, _):
        @pl.when(u < chunks)
        def _():
            sums(u)
            send_near(u)

        t = u - AHEAD

        @pl.when((t >= first) & (t < chunks))
        def _():
            send_far(t)

        v = u - 2 * AHEAD

        @pl.when((v >= first) & (v < chunks))
        def _():
            send_back(v)

        w = u - 3 * AHEAD

        @pl.when(w < first)
        def _():
            take_whole(w)

        @pl.when(w >= first)
        def _():
            take_back(w)

        norm(w)

        @pl.when(u == first)
        def _():
            for copy in small:
                copy.wait()
            own = (router_in[...] * gain_in[...]).astype(jnp.bfloat16)
            router_part[...] = own
            routers[group, me] = own
            for p in peers:
                remote(router_part, routers.at[group, me], router_send.at[0], router_recv.at[0], p).start()

        return 0

    lax.fori_loop(first, chunks + 3 * AHEAD, step, 0)

    seven = routers.at[group, pl.ds(0, fsdp - 1)]
    pltpu.make_async_copy(seven, seven, router_send.at[0]).wait()
    pltpu.make_async_copy(seven, seven, router_recv.at[0]).wait()
    for g in others:
        pltpu.make_async_remote_copy(
            routers.at[group], routers.at[group], router_send.at[1], router_recv.at[1],
            device_id={"ep": g}, device_id_type=MESH).start()
    three = routers.at[pl.ds(0, groups - 1)]
    pltpu.make_async_copy(three, three, router_send.at[1]).wait()
    pltpu.make_async_copy(three, three, router_recv.at[1]).wait()

    def last(t, _):
        drain(t)
        return 0

    lax.fori_loop(max(0, chunks - SLOTS), chunks, last, 0)
    for p in peers:
        column = final.at[:, :, pl.ds(pl.multiple_of(p * width, LANES), width)]
        pltpu.make_async_copy(column, column, block_recv.at[p]).wait()


def write(dims, final_in, scales_in, routers_in, final, scale, router, scale_part, router_part, sems):
    groups, fsdp, experts, steps, rows, width = dims
    columns = routers_in.shape[2]
    big = [pltpu.make_async_copy(final_in.at[e], final.at[e], sems.at[e]) for e in range(experts)]
    for copy in big:
        copy.start()
    for e in range(experts):
        parts = [scales_in[e * steps + s][:, :rows] for s in range(steps)]
        scale_part[e:e + 1, :] = jnp.concatenate(parts, axis=1)
    for g in range(groups):
        for d in range(fsdp):
            router_part[g * columns:(g + 1) * columns, d * width:(d + 1) * width] = routers_in[g, d]
    rest = [pltpu.make_async_copy(scale_part, scale, sems.at[experts]),
            pltpu.make_async_copy(router_part, router, sems.at[experts + 1])]
    for copy in rest:
        copy.start()
    for copy in big + rest:
        copy.wait()


def solution(mesh):
    groups, fsdp = mesh.shape["ep"], mesh.shape["fsdp"]

    def step(master, second, router, gain):
        experts, height, width = master.shape
        own = height // fsdp
        rows = largest_divisor(own, LANES, 8)
        steps = own // rows
        chunks, half = experts * steps, fsdp // 2
        first = min(3 * AHEAD, chunks)
        ring, wide = 3 * AHEAD + FETCH + 1, FETCH + 1
        columns = router.shape[1]
        hbm = pl.BlockSpec(memory_space=pltpu.HBM)
        inside = pl.BlockSpec(memory_space=pltpu.VMEM)
        dma = pltpu.SemaphoreType.DMA
        final, scales, routers = pl.pallas_call(
            functools.partial(exchange, (groups, fsdp, experts, steps, rows, width, first, ring, wide)),
            out_shape=(
                pltpu.VMEM((experts, own, fsdp * width), jnp.bfloat16),
                pltpu.VMEM((chunks, 1, LANES), jnp.float32),
                pltpu.VMEM((groups, fsdp, columns, width), jnp.bfloat16),
            ),
            in_specs=[hbm, hbm, hbm, hbm],
            out_specs=(inside, inside, inside),
            scratch_shapes=[
                pltpu.VMEM((ring, fsdp, rows, width), jnp.float32),
                pltpu.VMEM((wide, fsdp, rows, width), jnp.bfloat16),
                pltpu.VMEM((chunks, half, 2, LANES), jnp.float32),
                pltpu.VMEM((first, fsdp, half, 2, LANES), jnp.float32),
                pltpu.VMEM((chunks, half, 2, LANES), jnp.float32),
                pltpu.VMEM((chunks, 2, 2, LANES), jnp.float32),
                pltpu.VMEM((chunks, half, 2, LANES), jnp.float32),
                pltpu.VMEM((SLOTS, fsdp, rows, width), jnp.bfloat16),
                pltpu.VMEM((columns, width), jnp.float32),
                pltpu.VMEM((1, width), jnp.float32),
                pltpu.VMEM((columns, width), jnp.bfloat16),
                dma((ring,)), dma((wide,)), dma((2,)),
                dma((first,)), dma((first,)),
                dma((chunks,)), dma((chunks,)), dma((chunks,)), dma((chunks,)), dma((chunks,)), dma((chunks,)),
                dma((SLOTS,)), dma((fsdp,)), dma((2,)), dma((2,)),
            ],
            compiler_params=pltpu.CompilerParams(
                collective_id=0, has_side_effects=True, vmem_limit_bytes=28 * 2**20),
        )(
            master.reshape(experts, fsdp, own, width),
            second.reshape(experts, fsdp, own, width),
            pltpu.with_memory_space_constraint(router.T, pltpu.HBM),
            pltpu.with_memory_space_constraint(gain[None, :], pltpu.HBM),
        )
        final, scale, router = pl.pallas_call(
            functools.partial(write, (groups, fsdp, experts, steps, rows, width)),
            out_shape=(
                jax.ShapeDtypeStruct((experts, own, fsdp * width), jnp.bfloat16),
                jax.ShapeDtypeStruct((experts, own), jnp.float32),
                jax.ShapeDtypeStruct((groups * columns, fsdp * width), jnp.bfloat16),
            ),
            in_specs=[inside, inside, inside],
            out_specs=(hbm, hbm, hbm),
            scratch_shapes=[
                pltpu.VMEM((experts, own), jnp.float32),
                pltpu.VMEM((groups * columns, fsdp * width), jnp.bfloat16),
                dma((experts + 2,)),
            ],
            compiler_params=pltpu.CompilerParams(vmem_limit_bytes=2 * 2**20),
        )(final, scales, routers)
        return final, scale, router.T

    return jax.shard_map(
        step,
        mesh=mesh,
        in_specs=(P("ep", None, "fsdp"), P("ep", None, "fsdp"), P("fsdp", "ep"), P("fsdp")),
        out_specs=(P("ep", "fsdp", None), P("ep", "fsdp"), P()),
        check_vma=False,
    )
```

```python
import functools

import jax
import jax.numpy as jnp
from jax import lax
from jax.experimental import pallas as pl
from jax.experimental.pallas import tpu as pltpu
from jax.sharding import PartitionSpec as P

MESH = pl.DeviceIdType.MESH
LANES = 128
AHEAD = 2
SLOTS = 4
FETCH = 3
LATE = (5, 3)


def largest_divisor(size, limit, step):
    return max(d for d in range(step, limit + 1, step) if size % d == 0)


def exchange(dims, spans, first, *refs):
    groups, fsdp, steps, rows, width, ring, wide = dims
    if first:
        master, second, router, gain, final, scales, routers, *refs = refs
        router_in, gain_in, router_part, whole, small_sem, whole_send, whole_recv, router_send, router_recv, *refs = refs
    else:
        master, second, _, final, scales, *refs = refs
    (held, narrow, part, gathered, cross, inverse, sent, master_sem, second_sem, near_send, near_recv,
     far_send, far_recv, back_send, back_recv, block_send, block_recv) = refs
    half = fsdp // 2
    me, group = lax.axis_index("fsdp"), lax.axis_index("ep")
    core = lax.rem(group, 2)
    low = jnp.where(core == 0, spans[0][0], spans[1][0])
    chunks = jnp.where(core == 0, spans[0][1], spans[1][1]) - low
    side, lane = me // half, lax.rem(me, half)
    peers = [lax.rem(me + k, fsdp) for k in range(1, fsdp)]
    near = [lax.rem(lane + k, half) for k in range(1, half)]
    others = [lax.rem(group + k, groups) for k in range(1, groups)]
    partner = lax.rem(me + half, fsdp)

    def load(t):
        e, s = (low + t) // steps, lax.rem(low + t, steps)
        span = pl.ds(pl.multiple_of(s * rows, 8), rows)
        a, b = lax.rem(t, ring), lax.rem(t, wide)
        return (
            pltpu.make_async_copy(master.at[e, :, span, :], held.at[a], master_sem.at[a]),
            pltpu.make_async_copy(second.at[e, :, span, :], narrow.at[b], second_sem.at[b]),
        )

    for t in range(FETCH):
        for copy in load(t):
            copy.start()
    small = ()
    if first:
        small = (pltpu.make_async_copy(router, router_in, small_sem.at[0]),
                 pltpu.make_async_copy(gain, gain_in, small_sem.at[1]))
    for copy in small:
        copy.start()

    barrier = pltpu.get_barrier_semaphore()
    for p in peers:
        pl.semaphore_signal(barrier, inc=1, device_id={"fsdp": p}, device_id_type=MESH)
    if first:
        for g in others:
            pl.semaphore_signal(barrier, inc=1, device_id={"ep": g}, device_id_type=MESH)

    def remote(source, target, send, recv, p):
        return pltpu.make_async_remote_copy(
            source, target, send, recv, device_id={"fsdp": p}, device_id_type=MESH)

    def sums(t):
        for copy in load(t):
            copy.wait()
        a, b = lax.rem(t, ring), lax.rem(t, wide)

        def body(j, _):
            for s in range(2):
                d = s * half + j
                x = held[a, d] + narrow[b, d].astype(jnp.float32)
                held[a, d] = x
                x = x * x
                acc = x[:, :LANES]
                for c in range(LANES, width, LANES):
                    acc = acc + x[:, c:c + LANES]
                if rows < LANES:
                    acc = jnp.concatenate([acc, jnp.zeros((LANES - rows, LANES), jnp.float32)], axis=0)
                part[t, j, pl.ds(s, 1), :] = jnp.sum(acc.T, axis=0, keepdims=True)
            return 0

        lax.fori_loop(0, half, body, 0)

        @pl.when(t + FETCH < chunks)
        def _():
            for copy in load(t + FETCH):
                copy.start()

    def send_whole(t):
        whole[t, me] = part[t]
        for p in peers:
            remote(part.at[t], whole.at[t, me], whole_send.at[t], whole_recv.at[t], p).start()

    def send_near(t):
        gathered[t, lane] = part[t, lane]
        for q in near:
            remote(part.at[t, q], gathered.at[t, lane], near_send.at[t], near_recv.at[t], side * half + q).start()

    def many(ref, t, count, sem):
        block = ref.at[t, pl.ds(0, count)]
        return pltpu.make_async_copy(block, block, sem)

    def put_scale(t, scale):
        scales[t] = jnp.where(side == 0, scale[0:1], scale[1:2])

    def send_far(t):
        many(gathered, t, half - 1, near_recv.at[t]).wait()
        cross[t, side] = jnp.sum(gathered[t], axis=0)
        remote(cross.at[t, side], cross.at[t, side], far_send.at[t], far_recv.at[t], partner).start()

    def send_back(t):
        many(cross, t, 1, far_recv.at[t]).wait()
        scale = jnp.sqrt(cross[t, 0] + cross[t, 1])
        put_scale(t, scale)
        inverse[t, lane] = 1.0 / scale
        for q in near:
            remote(inverse.at[t, lane], inverse.at[t, lane], back_send.at[t], back_recv.at[t], side * half + q).start()

    def take_whole(t):
        many(whole, t, fsdp - 1, whole_recv.at[t]).wait()
        total = whole[t, 0]
        for k in range(1, fsdp):
            total = total + whole[t, k]
        scale = jnp.sqrt(total)
        inverse[t] = 1.0 / scale
        gathered[0] = scale
        put_scale(t, gathered[0, lane])
        many(whole, t, fsdp - 1, whole_send.at[t]).wait()

    def take_back(t):
        many(inverse, t, half - 1, back_recv.at[t]).wait()
        many(gathered, t, half - 1, near_send.at[t]).wait()
        many(cross, t, 1, far_send.at[t]).wait()
        many(inverse, t, half - 1, back_send.at[t]).wait()

    def drain(t):
        many(sent, lax.rem(t, SLOTS), fsdp - 1, block_send.at[lax.rem(t, SLOTS)]).wait()

    def norm(t):
        @pl.when(t >= SLOTS)
        def _():
            drain(t - SLOTS)

        a, out = lax.rem(t, ring), lax.rem(t, SLOTS)
        mine = pl.ds(pl.multiple_of(me * width, LANES), width)
        place = final.at[t, :, mine]

        def block(d):
            row = inverse[t, lax.rem(d, half), pl.ds(d // half, 1), :]
            factor = jnp.broadcast_to(row, (LANES, LANES)).T[:rows]
            for c in range(0, width, LANES):
                sent[out, d, :, c:c + LANES] = (held[a, d, :, c:c + LANES] * factor).astype(jnp.bfloat16)

        def push(d):
            remote(sent.at[out, d], place, block_send.at[out], block_recv.at[me], d).start()

        def body(k, _):
            block(lax.rem(me + k, fsdp))

            @pl.when(k > 1)
            def _():
                push(lax.rem(me + k - 1, fsdp))

            return 0

        lax.fori_loop(1, fsdp, body, 0)
        block(me)
        push(lax.rem(me + fsdp - 1, fsdp))
        final[t, :, mine] = sent[out, me]

    if first:
        sums(0)
        pl.semaphore_wait(barrier, len(peers) + len(others))
    else:
        pl.semaphore_wait(barrier, len(peers))

    def start(t, _):
        @pl.when(t > 0)
        def _():
            sums(t)

        send_whole(t)
        return 0

    if first:
        lax.fori_loop(0, first, start, 0)
        for copy in small:
            copy.wait()
        own = (router_in[...] * gain_in[...]).astype(jnp.bfloat16)
        router_part[...] = own
        routers[group, me] = own
        for p in peers:
            remote(router_part, routers.at[group, me], router_send.at[0], router_recv.at[0], p).start()

    def step(u, _):
        @pl.when(u < chunks)
        def _():
            sums(u)
            send_near(u)

        t = u - AHEAD

        @pl.when((t >= first) & (t < chunks))
        def _():
            send_far(t)

        v = u - 2 * AHEAD

        @pl.when((v >= first) & (v < chunks))
        def _():
            send_back(v)

        w = u - 3 * AHEAD

        if first:
            @pl.when(w < first)
            def _():
                take_whole(w)

        @pl.when(w >= first)
        def _():
            take_back(w)

        @pl.when(w >= 0)
        def _():
            norm(w)

        return 0

    lax.fori_loop(first, chunks + 3 * AHEAD, step, 0)

    if first:
        seven = routers.at[group, pl.ds(0, fsdp - 1)]
        pltpu.make_async_copy(seven, seven, router_send.at[0]).wait()
        pltpu.make_async_copy(seven, seven, router_recv.at[0]).wait()
        for g in others:
            pltpu.make_async_remote_copy(
                routers.at[group], routers.at[group], router_send.at[1], router_recv.at[1],
                device_id={"ep": g}, device_id_type=MESH).start()
        three = routers.at[pl.ds(0, groups - 1)]
        pltpu.make_async_copy(three, three, router_send.at[1]).wait()
        pltpu.make_async_copy(three, three, router_recv.at[1]).wait()

    def last(t, _):
        drain(t)
        return 0

    lax.fori_loop(chunks - SLOTS, chunks, last, 0)
    for c, (start_at, end_at) in enumerate(spans):
        @pl.when(core == c)
        def _(count=end_at - start_at):
            for p in peers:
                column = final.at[pl.ds(0, count), :, pl.ds(pl.multiple_of(p * width, LANES), width)]
                pltpu.make_async_copy(column, column, block_recv.at[p]).wait()


def write_first(cuts, steps, final_in, routers_in, final, router, router_part, sems):
    groups, fsdp, columns, width = routers_in.shape
    core = lax.rem(lax.axis_index("ep"), 2)
    for g in range(groups):
        for d in range(fsdp):
            router_part[g * columns:(g + 1) * columns, d * width:(d + 1) * width] = routers_in[g, d]
    rest = pltpu.make_async_copy(router_part, router, sems.at[0])
    rest.start()
    for c, cut in enumerate(cuts):
        @pl.when(core == c)
        def _(cut=cut):
            ends = list(range(0, cut, steps)) + [cut]
            copies = []
            for k, (a, b) in enumerate(zip(ends, ends[1:])):
                span = pl.ds(a, b - a)
                copies.append(pltpu.make_async_copy(final_in.at[span], final.at[span], sems.at[k + 1]))
            for copy in copies:
                copy.start()
            for copy in copies:
                copy.wait()
    rest.wait()


def write_second(cuts, total, steps, _, late_in, scales_in, late_scales_in, final, scale, scale_part, sems):
    rows = final.shape[1]
    core = lax.rem(lax.axis_index("ep"), 2)
    for c, cut in enumerate(cuts):
        @pl.when(core == c)
        def _(cut=cut):
            big = pltpu.make_async_copy(late_in.at[pl.ds(0, total - cut)], final.at[pl.ds(cut, total - cut)], sems.at[0])
            big.start()
            for e in range(total // steps):
                parts = []
                for t in range(e * steps, (e + 1) * steps):
                    row = scales_in[t] if t < cut else late_scales_in[t - cut]
                    parts.append(row[:, :rows])
                scale_part[e:e + 1, :] = jnp.concatenate(parts, axis=1)
            small = pltpu.make_async_copy(scale_part, scale, sems.at[1])
            small.start()
            big.wait()
            small.wait()


def solution(mesh):
    groups, fsdp = mesh.shape["ep"], mesh.shape["fsdp"]

    def step(master, second, router, gain):
        experts, height, width = master.shape
        own = height // fsdp
        rows = largest_divisor(own, LANES, 8)
        steps = own // rows
        chunks, half = experts * steps, fsdp // 2
        ring, wide = 3 * AHEAD + FETCH + 1, FETCH + 1
        columns = router.shape[1]
        cuts = [chunks - max(chunks // late, SLOTS) for late in LATE]
        hbm = pl.BlockSpec(memory_space=pltpu.HBM)
        inside = pl.BlockSpec(memory_space=pltpu.VMEM)
        dma = pltpu.SemaphoreType.DMA
        dims = (groups, fsdp, steps, rows, width, ring, wide)

        def scratch(count):
            table = (count, half, 2, LANES)
            return [
                pltpu.VMEM((ring, fsdp, rows, width), jnp.float32),
                pltpu.VMEM((wide, fsdp, rows, width), jnp.bfloat16),
                pltpu.VMEM(table, jnp.float32),
                pltpu.VMEM(table, jnp.float32),
                pltpu.VMEM((count, 2, 2, LANES), jnp.float32),
                pltpu.VMEM(table, jnp.float32),
                pltpu.VMEM((SLOTS, fsdp, rows, width), jnp.bfloat16),
                dma((ring,)), dma((wide,)),
                dma((count,)), dma((count,)), dma((count,)), dma((count,)), dma((count,)), dma((count,)),
                dma((SLOTS,)), dma((fsdp,)),
            ]

        def grant(mebibytes, ident=None):
            if ident is None:
                return pltpu.CompilerParams(vmem_limit_bytes=mebibytes * 2**20)
            return pltpu.CompilerParams(
                collective_id=ident, has_side_effects=True, vmem_limit_bytes=mebibytes * 2**20)

        whole = jax.ShapeDtypeStruct((chunks, rows, fsdp * width), jnp.bfloat16)
        master = master.reshape(experts, fsdp, own, width)
        second = second.reshape(experts, fsdp, own, width)
        most, first = max(cuts), 3 * AHEAD
        early, scales, routers = pl.pallas_call(
            functools.partial(exchange, dims, [(0, cut) for cut in cuts], first),
            out_shape=(
                pltpu.VMEM((most, rows, fsdp * width), jnp.bfloat16),
                pltpu.VMEM((most, 1, LANES), jnp.float32),
                pltpu.VMEM((groups, fsdp, columns, width), jnp.bfloat16),
            ),
            in_specs=[hbm, hbm, hbm, hbm],
            out_specs=(inside, inside, inside),
            scratch_shapes=[
                pltpu.VMEM((columns, width), jnp.float32),
                pltpu.VMEM((1, width), jnp.float32),
                pltpu.VMEM((columns, width), jnp.bfloat16),
                pltpu.VMEM((first, fsdp, half, 2, LANES), jnp.float32),
                dma((2,)), dma((first,)), dma((first,)), dma((2,)), dma((2,)),
            ] + scratch(most),
            compiler_params=grant(28, 0),
            name="exchange_early",
        )(
            master,
            second,
            pltpu.with_memory_space_constraint(router.T, pltpu.HBM),
            pltpu.with_memory_space_constraint(gain[None, :], pltpu.HBM),
        )
        final, router = pl.pallas_call(
            functools.partial(write_first, cuts, steps),
            out_shape=(whole, jax.ShapeDtypeStruct((groups * columns, fsdp * width), jnp.bfloat16)),
            in_specs=[inside, inside],
            out_specs=(hbm, hbm),
            scratch_shapes=[
                pltpu.VMEM((groups * columns, fsdp * width), jnp.bfloat16),
                dma((experts + 2,)),
            ],
            compiler_params=grant(2),
            name="write_early",
        )(early, routers)
        most = chunks - min(cuts)
        late, late_scales = pl.pallas_call(
            functools.partial(exchange, dims, [(cut, chunks) for cut in cuts], 0),
            out_shape=(
                pltpu.VMEM((most, rows, fsdp * width), jnp.bfloat16),
                pltpu.VMEM((most, 1, LANES), jnp.float32),
            ),
            in_specs=[hbm, hbm, hbm],
            out_specs=(inside, inside),
            scratch_shapes=scratch(most),
            compiler_params=grant(28, 1),
            name="exchange_late",
        )(master, second, pltpu.with_memory_space_constraint(router, pltpu.HBM))
        final, scale = pl.pallas_call(
            functools.partial(write_second, cuts, chunks, steps),
            out_shape=(whole, jax.ShapeDtypeStruct((experts, own), jnp.float32)),
            in_specs=[hbm, inside, inside, inside],
            out_specs=(hbm, hbm),
            scratch_shapes=[pltpu.VMEM((experts, own), jnp.float32), dma((2,))],
            input_output_aliases={0: 0},
            compiler_params=grant(2),
            name="write_late",
        )(final, late, scales, late_scales)
        return final.reshape(experts, own, fsdp * width), scale, router.T

    return jax.shard_map(
        step,
        mesh=mesh,
        in_specs=(P("ep", None, "fsdp"), P("ep", None, "fsdp"), P("fsdp", "ep"), P("fsdp")),
        out_specs=(P("ep", "fsdp", None), P("ep", "fsdp"), P()),
        check_vma=False,
    )
```

```python
import functools

import jax
import jax.numpy as jnp
from jax import lax
from jax.experimental import pallas as pl
from jax.experimental.pallas import tpu as pltpu
from jax.sharding import PartitionSpec as P

MESH = pl.DeviceIdType.MESH
LANES = 128
AHEAD = 2
SLOTS = 4
FETCH = 3
LATE = (10, 4)


def largest_divisor(size, limit, step):
    return max(d for d in range(step, limit + 1, step) if size % d == 0)


def exchange(dims, spans, first, *refs):
    groups, fsdp, steps, rows, width, ring, wide = dims
    if first:
        master, second, router, gain, final, scales, routers, *refs = refs
        router_in, gain_in, router_part, whole, small_sem, whole_send, whole_recv, router_send, router_recv, *refs = refs
    else:
        master, second, _, final, scales, *refs = refs
    (held, narrow, part, gathered, cross, inverse, sent, master_sem, second_sem, near_send, near_recv,
     far_send, far_recv, back_send, back_recv, block_send, block_recv) = refs
    half = fsdp // 2
    me, group = lax.axis_index("fsdp"), lax.axis_index("ep")
    core = lax.rem(group, 2)
    low = jnp.where(core == 0, spans[0][0], spans[1][0])
    chunks = jnp.where(core == 0, spans[0][1], spans[1][1]) - low
    side, lane = me // half, lax.rem(me, half)
    peers = [lax.rem(me + k, fsdp) for k in range(1, fsdp)]
    near = [lax.rem(lane + k, half) for k in range(1, half)]
    others = [lax.rem(group + k, groups) for k in range(1, groups)]
    partner = lax.rem(me + half, fsdp)

    def load(t):
        e, s = (low + t) // steps, lax.rem(low + t, steps)
        span = pl.ds(pl.multiple_of(s * rows, 8), rows)
        a, b = lax.rem(t, ring), lax.rem(t, wide)
        return (
            pltpu.make_async_copy(master.at[e, :, span, :], held.at[a], master_sem.at[a]),
            pltpu.make_async_copy(second.at[e, :, span, :], narrow.at[b], second_sem.at[b]),
        )

    for t in range(FETCH):
        for copy in load(t):
            copy.start()
    small = ()
    if first:
        small = (pltpu.make_async_copy(router, router_in, small_sem.at[0]),
                 pltpu.make_async_copy(gain, gain_in, small_sem.at[1]))
    for copy in small:
        copy.start()

    barrier = pltpu.get_barrier_semaphore()
    for p in peers:
        pl.semaphore_signal(barrier, inc=1, device_id={"fsdp": p}, device_id_type=MESH)
    if first:
        for g in others:
            pl.semaphore_signal(barrier, inc=1, device_id={"ep": g}, device_id_type=MESH)

    def remote(source, target, send, recv, p):
        return pltpu.make_async_remote_copy(
            source, target, send, recv, device_id={"fsdp": p}, device_id_type=MESH)

    def sums(t):
        for copy in load(t):
            copy.wait()
        a, b = lax.rem(t, ring), lax.rem(t, wide)

        def body(j, _):
            for s in range(2):
                d = s * half + j
                x = held[a, d] + narrow[b, d].astype(jnp.float32)
                held[a, d] = x
                x = x * x
                acc = x[:, :LANES]
                for c in range(LANES, width, LANES):
                    acc = acc + x[:, c:c + LANES]
                if rows < LANES:
                    acc = jnp.concatenate([acc, jnp.zeros((LANES - rows, LANES), jnp.float32)], axis=0)
                part[t, j, pl.ds(s, 1), :] = jnp.sum(acc.T, axis=0, keepdims=True)
            return 0

        lax.fori_loop(0, half, body, 0)

        @pl.when(t + FETCH < chunks)
        def _():
            for copy in load(t + FETCH):
                copy.start()

    def send_whole(t):
        whole[t, me] = part[t]
        for p in peers:
            remote(part.at[t], whole.at[t, me], whole_send.at[t], whole_recv.at[t], p).start()

    def send_near(t):
        gathered[t, lane] = part[t, lane]
        for q in near:
            remote(part.at[t, q], gathered.at[t, lane], near_send.at[t], near_recv.at[t], side * half + q).start()

    def many(ref, t, count, sem):
        block = ref.at[t, pl.ds(0, count)]
        return pltpu.make_async_copy(block, block, sem)

    def put_scale(t, scale):
        scales[t] = jnp.where(side == 0, scale[0:1], scale[1:2])

    def send_far(t):
        many(gathered, t, half - 1, near_recv.at[t]).wait()
        cross[t, side] = jnp.sum(gathered[t], axis=0)
        remote(cross.at[t, side], cross.at[t, side], far_send.at[t], far_recv.at[t], partner).start()

    def send_back(t):
        many(cross, t, 1, far_recv.at[t]).wait()
        scale = jnp.sqrt(cross[t, 0] + cross[t, 1])
        put_scale(t, scale)
        inverse[t, lane] = 1.0 / scale
        for q in near:
            remote(inverse.at[t, lane], inverse.at[t, lane], back_send.at[t], back_recv.at[t], side * half + q).start()

    def take_whole(t):
        many(whole, t, fsdp - 1, whole_recv.at[t]).wait()
        total = whole[t, 0]
        for k in range(1, fsdp):
            total = total + whole[t, k]
        scale = jnp.sqrt(total)
        inverse[t] = 1.0 / scale
        gathered[0] = scale
        put_scale(t, gathered[0, lane])
        many(whole, t, fsdp - 1, whole_send.at[t]).wait()

    def take_back(t):
        many(inverse, t, half - 1, back_recv.at[t]).wait()
        many(gathered, t, half - 1, near_send.at[t]).wait()
        many(cross, t, 1, far_send.at[t]).wait()
        many(inverse, t, half - 1, back_send.at[t]).wait()

    def drain(t):
        many(sent, lax.rem(t, SLOTS), fsdp - 1, block_send.at[lax.rem(t, SLOTS)]).wait()

    def norm(t):
        @pl.when(t >= SLOTS)
        def _():
            drain(t - SLOTS)

        a, out = lax.rem(t, ring), lax.rem(t, SLOTS)
        mine = pl.ds(pl.multiple_of(me * width, LANES), width)
        place = final.at[t, :, mine]

        def block(d):
            row = inverse[t, lax.rem(d, half), pl.ds(d // half, 1), :]
            factor = jnp.broadcast_to(row, (LANES, LANES)).T[:rows]
            for c in range(0, width, LANES):
                sent[out, d, :, c:c + LANES] = (held[a, d, :, c:c + LANES] * factor).astype(jnp.bfloat16)

        def push(d):
            remote(sent.at[out, d], place, block_send.at[out], block_recv.at[me], d).start()

        def body(k, _):
            block(lax.rem(me + k, fsdp))

            @pl.when(k > 1)
            def _():
                push(lax.rem(me + k - 1, fsdp))

            return 0

        lax.fori_loop(1, fsdp, body, 0)
        block(me)
        push(lax.rem(me + fsdp - 1, fsdp))
        final[t, :, mine] = sent[out, me]

    if first:
        sums(0)
        pl.semaphore_wait(barrier, len(peers) + len(others))
    else:
        pl.semaphore_wait(barrier, len(peers))

    def start(t, _):
        @pl.when(t > 0)
        def _():
            sums(t)

        send_whole(t)
        return 0

    if first:
        lax.fori_loop(0, first, start, 0)
        for copy in small:
            copy.wait()
        own = (router_in[...] * gain_in[...]).astype(jnp.bfloat16)
        router_part[...] = own
        routers[group, me] = own
        for p in peers:
            remote(router_part, routers.at[group, me], router_send.at[0], router_recv.at[0], p).start()

    def send_router():
        seven = routers.at[group, pl.ds(0, fsdp - 1)]
        pltpu.make_async_copy(seven, seven, router_send.at[0]).wait()
        pltpu.make_async_copy(seven, seven, router_recv.at[0]).wait()
        for g in others:
            pltpu.make_async_remote_copy(
                routers.at[group], routers.at[group], router_send.at[1], router_recv.at[1],
                device_id={"ep": g}, device_id_type=MESH).start()

    def step(u, _):
        @pl.when(u < chunks)
        def _():
            sums(u)
            send_near(u)

        t = u - AHEAD

        @pl.when((t >= first) & (t < chunks))
        def _():
            send_far(t)

        v = u - 2 * AHEAD

        @pl.when((v >= first) & (v < chunks))
        def _():
            send_back(v)

        w = u - 3 * AHEAD

        if first:
            @pl.when(w < first)
            def _():
                take_whole(w)

        @pl.when(w >= first)
        def _():
            take_back(w)

        @pl.when(w >= 0)
        def _():
            norm(w)

        if first:
            @pl.when(w == SLOTS)
            def _():
                send_router()

        return 0

    lax.fori_loop(first, chunks + 3 * AHEAD, step, 0)

    if first:
        three = routers.at[pl.ds(0, groups - 1)]
        pltpu.make_async_copy(three, three, router_send.at[1]).wait()
        pltpu.make_async_copy(three, three, router_recv.at[1]).wait()

    def last(t, _):
        drain(t)
        return 0

    lax.fori_loop(chunks - SLOTS, chunks, last, 0)
    for c, (start_at, end_at) in enumerate(spans):
        @pl.when(core == c)
        def _(count=end_at - start_at):
            for p in peers:
                column = final.at[pl.ds(0, count), :, pl.ds(pl.multiple_of(p * width, LANES), width)]
                pltpu.make_async_copy(column, column, block_recv.at[p]).wait()


def write_first(cuts, steps, final_in, routers_in, final, router, router_part, sems):
    groups, fsdp, columns, width = routers_in.shape
    core = lax.rem(lax.axis_index("ep"), 2)
    for g in range(groups):
        for d in range(fsdp):
            router_part[g * columns:(g + 1) * columns, d * width:(d + 1) * width] = routers_in[g, d]
    rest = pltpu.make_async_copy(router_part, router, sems.at[0])
    rest.start()
    for c, cut in enumerate(cuts):
        @pl.when(core == c)
        def _(cut=cut):
            ends = list(range(0, cut, steps)) + [cut]
            copies = []
            for k, (a, b) in enumerate(zip(ends, ends[1:])):
                span = pl.ds(a, b - a)
                copies.append(pltpu.make_async_copy(final_in.at[span], final.at[span], sems.at[k + 1]))
            for copy in copies:
                copy.start()
            for copy in copies:
                copy.wait()
    rest.wait()


def write_second(cuts, total, steps, _, late_in, scales_in, late_scales_in, final, scale, scale_part, sems):
    rows = final.shape[1]
    core = lax.rem(lax.axis_index("ep"), 2)
    for c, cut in enumerate(cuts):
        @pl.when(core == c)
        def _(cut=cut):
            big = pltpu.make_async_copy(late_in.at[pl.ds(0, total - cut)], final.at[pl.ds(cut, total - cut)], sems.at[0])
            big.start()
            for e in range(total // steps):
                parts = []
                for t in range(e * steps, (e + 1) * steps):
                    row = scales_in[t] if t < cut else late_scales_in[t - cut]
                    parts.append(row[:, :rows])
                scale_part[e:e + 1, :] = jnp.concatenate(parts, axis=1)
            small = pltpu.make_async_copy(scale_part, scale, sems.at[1])
            small.start()
            big.wait()
            small.wait()


def solution(mesh):
    groups, fsdp = mesh.shape["ep"], mesh.shape["fsdp"]

    def step(master, second, router, gain):
        experts, height, width = master.shape
        own = height // fsdp
        rows = largest_divisor(own, LANES, 8)
        steps = own // rows
        chunks, half = experts * steps, fsdp // 2
        ring, wide = 3 * AHEAD + FETCH + 1, FETCH + 1
        columns = router.shape[1]
        cuts = [chunks - max(chunks // late, SLOTS) for late in LATE]
        hbm = pl.BlockSpec(memory_space=pltpu.HBM)
        inside = pl.BlockSpec(memory_space=pltpu.VMEM)
        dma = pltpu.SemaphoreType.DMA
        dims = (groups, fsdp, steps, rows, width, ring, wide)

        def scratch(count):
            table = (count, half, 2, LANES)
            return [
                pltpu.VMEM((ring, fsdp, rows, width), jnp.float32),
                pltpu.VMEM((wide, fsdp, rows, width), jnp.bfloat16),
                pltpu.VMEM(table, jnp.float32),
                pltpu.VMEM(table, jnp.float32),
                pltpu.VMEM((count, 2, 2, LANES), jnp.float32),
                pltpu.VMEM(table, jnp.float32),
                pltpu.VMEM((SLOTS, fsdp, rows, width), jnp.bfloat16),
                dma((ring,)), dma((wide,)),
                dma((count,)), dma((count,)), dma((count,)), dma((count,)), dma((count,)), dma((count,)),
                dma((SLOTS,)), dma((fsdp,)),
            ]

        def grant(mebibytes, ident=None):
            if ident is None:
                return pltpu.CompilerParams(vmem_limit_bytes=mebibytes * 2**20)
            return pltpu.CompilerParams(
                collective_id=ident, has_side_effects=True, vmem_limit_bytes=mebibytes * 2**20)

        whole = jax.ShapeDtypeStruct((chunks, rows, fsdp * width), jnp.bfloat16)
        master = master.reshape(experts, fsdp, own, width)
        second = second.reshape(experts, fsdp, own, width)
        most, first = max(cuts), 3 * AHEAD
        early, scales, routers = pl.pallas_call(
            functools.partial(exchange, dims, [(0, cut) for cut in cuts], first),
            out_shape=(
                pltpu.VMEM((most, rows, fsdp * width), jnp.bfloat16),
                pltpu.VMEM((most, 1, LANES), jnp.float32),
                pltpu.VMEM((groups, fsdp, columns, width), jnp.bfloat16),
            ),
            in_specs=[hbm, hbm, hbm, hbm],
            out_specs=(inside, inside, inside),
            scratch_shapes=[
                pltpu.VMEM((columns, width), jnp.float32),
                pltpu.VMEM((1, width), jnp.float32),
                pltpu.VMEM((columns, width), jnp.bfloat16),
                pltpu.VMEM((first, fsdp, half, 2, LANES), jnp.float32),
                dma((2,)), dma((first,)), dma((first,)), dma((2,)), dma((2,)),
            ] + scratch(most),
            compiler_params=grant(28, 0),
            name="exchange_early",
        )(
            master,
            second,
            pltpu.with_memory_space_constraint(router.T, pltpu.HBM),
            pltpu.with_memory_space_constraint(gain[None, :], pltpu.HBM),
        )
        final, router = pl.pallas_call(
            functools.partial(write_first, cuts, steps),
            out_shape=(whole, jax.ShapeDtypeStruct((groups * columns, fsdp * width), jnp.bfloat16)),
            in_specs=[inside, inside],
            out_specs=(hbm, hbm),
            scratch_shapes=[
                pltpu.VMEM((groups * columns, fsdp * width), jnp.bfloat16),
                dma((experts + 2,)),
            ],
            compiler_params=grant(2),
            name="write_early",
        )(early, routers)
        most = chunks - min(cuts)
        late, late_scales = pl.pallas_call(
            functools.partial(exchange, dims, [(cut, chunks) for cut in cuts], 0),
            out_shape=(
                pltpu.VMEM((most, rows, fsdp * width), jnp.bfloat16),
                pltpu.VMEM((most, 1, LANES), jnp.float32),
            ),
            in_specs=[hbm, hbm, hbm],
            out_specs=(inside, inside),
            scratch_shapes=scratch(most),
            compiler_params=grant(28, 1),
            name="exchange_late",
        )(master, second, pltpu.with_memory_space_constraint(router, pltpu.HBM))
        final, scale = pl.pallas_call(
            functools.partial(write_second, cuts, chunks, steps),
            out_shape=(whole, jax.ShapeDtypeStruct((experts, own), jnp.float32)),
            in_specs=[hbm, inside, inside, inside],
            out_specs=(hbm, hbm),
            scratch_shapes=[pltpu.VMEM((experts, own), jnp.float32), dma((2,))],
            input_output_aliases={0: 0},
            compiler_params=grant(2),
            name="write_late",
        )(final, late, scales, late_scales)
        return final.reshape(experts, own, fsdp * width), scale, router.T

    return jax.shard_map(
        step,
        mesh=mesh,
        in_specs=(P("ep", None, "fsdp"), P("ep", None, "fsdp"), P("fsdp", "ep"), P("fsdp")),
        out_specs=(P("ep", "fsdp", None), P("ep", "fsdp"), P()),
        check_vma=False,
    )
```

```python
import functools

import jax
import jax.numpy as jnp
from jax import lax
from jax.experimental import pallas as pl
from jax.experimental.pallas import tpu as pltpu
from jax.sharding import PartitionSpec as P

MESH = pl.DeviceIdType.MESH
LANES = 128
AHEAD = 2
SLOTS = 4
FETCH = 3
LATE = (10, 4)


def largest_divisor(size, limit, step):
    return max(d for d in range(step, limit + 1, step) if size % d == 0)


def exchange(dims, spans, first, *refs):
    groups, fsdp, steps, rows, width, ring, wide = dims
    if first:
        master, second, router, gain, final, scales, routers, *refs = refs
        router_in, gain_in, router_part, whole, small_sem, whole_send, whole_recv, router_send, router_recv, *refs = refs
    else:
        master, second, _, final, scales, *refs = refs
    (held, narrow, part, gathered, cross, inverse, sent, master_sem, second_sem, near_send, near_recv,
     far_send, far_recv, back_send, back_recv, block_send, block_recv) = refs
    half = fsdp // 2
    me, group = lax.axis_index("fsdp"), lax.axis_index("ep")
    core = lax.rem(group, 2)
    low = jnp.where(core == 0, spans[0][0], spans[1][0])
    chunks = jnp.where(core == 0, spans[0][1], spans[1][1]) - low
    side, lane = me // half, lax.rem(me, half)
    peers = [lax.rem(me + k, fsdp) for k in range(1, fsdp)]
    near = [lax.rem(lane + k, half) for k in range(1, half)]
    others = [lax.rem(group + k, groups) for k in range(1, groups)]
    partner = lax.rem(me + half, fsdp)

    def load(t):
        e, s = (low + t) // steps, lax.rem(low + t, steps)
        span = pl.ds(pl.multiple_of(s * rows, 8), rows)
        a, b = lax.rem(t, ring), lax.rem(t, wide)
        return (
            pltpu.make_async_copy(master.at[e, :, span, :], held.at[a], master_sem.at[a]),
            pltpu.make_async_copy(second.at[e, :, span, :], narrow.at[b], second_sem.at[b]),
        )

    for t in range(FETCH):
        for copy in load(t):
            copy.start()
    small = ()
    if first:
        small = (pltpu.make_async_copy(router, router_in, small_sem.at[0]),
                 pltpu.make_async_copy(gain, gain_in, small_sem.at[1]))
    for copy in small:
        copy.start()

    barrier = pltpu.get_barrier_semaphore()
    for p in peers:
        pl.semaphore_signal(barrier, inc=1, device_id={"fsdp": p}, device_id_type=MESH)
    if first:
        for g in others:
            pl.semaphore_signal(barrier, inc=1, device_id={"ep": g}, device_id_type=MESH)

    def remote(source, target, send, recv, p):
        return pltpu.make_async_remote_copy(
            source, target, send, recv, device_id={"fsdp": p}, device_id_type=MESH)

    def sums(t):
        for copy in load(t):
            copy.wait()
        a, b = lax.rem(t, ring), lax.rem(t, wide)

        def body(j, _):
            for s in range(2):
                d = s * half + j
                x = held[a, d] + narrow[b, d].astype(jnp.float32)
                held[a, d] = x
                x = x * x
                acc = x[:, :LANES]
                for c in range(LANES, width, LANES):
                    acc = acc + x[:, c:c + LANES]
                if rows < LANES:
                    acc = jnp.concatenate([acc, jnp.zeros((LANES - rows, LANES), jnp.float32)], axis=0)
                part[t, j, pl.ds(s, 1), :] = jnp.sum(acc.T, axis=0, keepdims=True)
            return 0

        lax.fori_loop(0, half, body, 0)

        @pl.when(t + FETCH < chunks)
        def _():
            for copy in load(t + FETCH):
                copy.start()

    def send_whole(t):
        whole[t, me] = part[t]
        for p in peers:
            remote(part.at[t], whole.at[t, me], whole_send.at[t], whole_recv.at[t], p).start()

    def send_near(t):
        gathered[t, lane] = part[t, lane]
        for q in near:
            remote(part.at[t, q], gathered.at[t, lane], near_send.at[t], near_recv.at[t], side * half + q).start()

    def many(ref, t, count, sem):
        block = ref.at[t, pl.ds(0, count)]
        return pltpu.make_async_copy(block, block, sem)

    def put_scale(t, scale):
        scales[t] = jnp.where(side == 0, scale[0:1], scale[1:2])

    def send_far(t):
        many(gathered, t, half - 1, near_recv.at[t]).wait()
        cross[t, side] = jnp.sum(gathered[t], axis=0)
        remote(cross.at[t, side], cross.at[t, side], far_send.at[t], far_recv.at[t], partner).start()

    def send_back(t):
        many(cross, t, 1, far_recv.at[t]).wait()
        scale = jnp.sqrt(cross[t, 0] + cross[t, 1])
        put_scale(t, scale)
        inverse[t, lane] = 1.0 / scale
        for q in near:
            remote(inverse.at[t, lane], inverse.at[t, lane], back_send.at[t], back_recv.at[t], side * half + q).start()

    def take_whole(t):
        many(whole, t, fsdp - 1, whole_recv.at[t]).wait()
        total = whole[t, 0]
        for k in range(1, fsdp):
            total = total + whole[t, k]
        scale = jnp.sqrt(total)
        inverse[t] = 1.0 / scale
        gathered[0] = scale
        put_scale(t, gathered[0, lane])
        many(whole, t, fsdp - 1, whole_send.at[t]).wait()

    def take_back(t):
        many(inverse, t, half - 1, back_recv.at[t]).wait()
        many(gathered, t, half - 1, near_send.at[t]).wait()
        many(cross, t, 1, far_send.at[t]).wait()
        many(inverse, t, half - 1, back_send.at[t]).wait()

    def drain(t):
        many(sent, lax.rem(t, SLOTS), fsdp - 1, block_send.at[lax.rem(t, SLOTS)]).wait()

    def norm(t):
        @pl.when(t >= SLOTS)
        def _():
            drain(t - SLOTS)

        a, out = lax.rem(t, ring), lax.rem(t, SLOTS)
        mine = pl.ds(pl.multiple_of(me * width, LANES), width)
        place = final.at[t, :, mine]

        def block(d):
            row = inverse[t, lax.rem(d, half), pl.ds(d // half, 1), :]
            factor = jnp.broadcast_to(row, (LANES, LANES)).T[:rows]
            for c in range(0, width, LANES):
                sent[out, d, :, c:c + LANES] = (held[a, d, :, c:c + LANES] * factor).astype(jnp.bfloat16)

        def push(d):
            remote(sent.at[out, d], place, block_send.at[out], block_recv.at[me], d).start()

        def body(k, _):
            block(lax.rem(me + k, fsdp))

            @pl.when(k > 1)
            def _():
                push(lax.rem(me + k - 1, fsdp))

            return 0

        lax.fori_loop(1, fsdp, body, 0)
        block(me)
        push(lax.rem(me + fsdp - 1, fsdp))
        final[t, :, mine] = sent[out, me]

    if first:
        sums(0)
        pl.semaphore_wait(barrier, len(peers) + len(others))
    else:
        pl.semaphore_wait(barrier, len(peers))

    def start(t, _):
        @pl.when(t > 0)
        def _():
            sums(t)

        send_whole(t)
        return 0

    if first:
        lax.fori_loop(0, first, start, 0)
        for copy in small:
            copy.wait()
        own = (router_in[...] * gain_in[...]).astype(jnp.bfloat16)
        router_part[...] = own
        routers[group, me] = own
        for p in peers:
            remote(router_part, routers.at[group, me], router_send.at[0], router_recv.at[0], p).start()

    def send_router():
        seven = routers.at[group, pl.ds(0, fsdp - 1)]
        pltpu.make_async_copy(seven, seven, router_send.at[0]).wait()
        pltpu.make_async_copy(seven, seven, router_recv.at[0]).wait()
        for g in others:
            pltpu.make_async_remote_copy(
                routers.at[group], routers.at[group], router_send.at[1], router_recv.at[1],
                device_id={"ep": g}, device_id_type=MESH).start()

    def step(u, _):
        w = u - 3 * AHEAD

        if first:
            @pl.when(w < first)
            def _():
                take_whole(w)

        @pl.when(w >= first)
        def _():
            take_back(w)

        @pl.when(w >= 0)
        def _():
            norm(w)

        @pl.when(u < chunks)
        def _():
            sums(u)
            send_near(u)

        t = u - AHEAD

        @pl.when((t >= first) & (t < chunks))
        def _():
            send_far(t)

        v = u - 2 * AHEAD

        @pl.when((v >= first) & (v < chunks))
        def _():
            send_back(v)

        if first:
            @pl.when(w == SLOTS)
            def _():
                send_router()

        return 0

    lax.fori_loop(first, chunks + 3 * AHEAD, step, 0)

    if first:
        three = routers.at[pl.ds(0, groups - 1)]
        pltpu.make_async_copy(three, three, router_send.at[1]).wait()
        pltpu.make_async_copy(three, three, router_recv.at[1]).wait()

    def last(t, _):
        drain(t)
        return 0

    lax.fori_loop(chunks - SLOTS, chunks, last, 0)
    for c, (start_at, end_at) in enumerate(spans):
        @pl.when(core == c)
        def _(count=end_at - start_at):
            for p in peers:
                column = final.at[pl.ds(0, count), :, pl.ds(pl.multiple_of(p * width, LANES), width)]
                pltpu.make_async_copy(column, column, block_recv.at[p]).wait()


def write_first(cuts, steps, final_in, routers_in, final, router, router_part, sems):
    groups, fsdp, columns, width = routers_in.shape
    core = lax.rem(lax.axis_index("ep"), 2)
    for g in range(groups):
        for d in range(fsdp):
            router_part[g * columns:(g + 1) * columns, d * width:(d + 1) * width] = routers_in[g, d]
    rest = pltpu.make_async_copy(router_part, router, sems.at[0])
    rest.start()
    for c, cut in enumerate(cuts):
        @pl.when(core == c)
        def _(cut=cut):
            ends = list(range(0, cut, steps)) + [cut]
            copies = []
            for k, (a, b) in enumerate(zip(ends, ends[1:])):
                span = pl.ds(a, b - a)
                copies.append(pltpu.make_async_copy(final_in.at[span], final.at[span], sems.at[k + 1]))
            for copy in copies:
                copy.start()
            for copy in copies:
                copy.wait()
    rest.wait()


def write_second(cuts, total, steps, _, late_in, scales_in, late_scales_in, final, scale, scale_part, sems):
    rows = final.shape[1]
    core = lax.rem(lax.axis_index("ep"), 2)
    for c, cut in enumerate(cuts):
        @pl.when(core == c)
        def _(cut=cut):
            big = pltpu.make_async_copy(late_in.at[pl.ds(0, total - cut)], final.at[pl.ds(cut, total - cut)], sems.at[0])
            big.start()
            for e in range(total // steps):
                parts = []
                for t in range(e * steps, (e + 1) * steps):
                    row = scales_in[t] if t < cut else late_scales_in[t - cut]
                    parts.append(row[:, :rows])
                scale_part[e:e + 1, :] = jnp.concatenate(parts, axis=1)
            small = pltpu.make_async_copy(scale_part, scale, sems.at[1])
            small.start()
            big.wait()
            small.wait()


def solution(mesh):
    groups, fsdp = mesh.shape["ep"], mesh.shape["fsdp"]

    def step(master, second, router, gain):
        experts, height, width = master.shape
        own = height // fsdp
        rows = largest_divisor(own, LANES, 8)
        steps = own // rows
        chunks, half = experts * steps, fsdp // 2
        ring, wide = 3 * AHEAD + FETCH + 1, FETCH + 1
        columns = router.shape[1]
        cuts = [chunks - max(chunks // late, SLOTS) for late in LATE]
        hbm = pl.BlockSpec(memory_space=pltpu.HBM)
        inside = pl.BlockSpec(memory_space=pltpu.VMEM)
        dma = pltpu.SemaphoreType.DMA
        dims = (groups, fsdp, steps, rows, width, ring, wide)

        def scratch(count):
            table = (count, half, 2, LANES)
            return [
                pltpu.VMEM((ring, fsdp, rows, width), jnp.float32),
                pltpu.VMEM((wide, fsdp, rows, width), jnp.bfloat16),
                pltpu.VMEM(table, jnp.float32),
                pltpu.VMEM(table, jnp.float32),
                pltpu.VMEM((count, 2, 2, LANES), jnp.float32),
                pltpu.VMEM(table, jnp.float32),
                pltpu.VMEM((SLOTS, fsdp, rows, width), jnp.bfloat16),
                dma((ring,)), dma((wide,)),
                dma((count,)), dma((count,)), dma((count,)), dma((count,)), dma((count,)), dma((count,)),
                dma((SLOTS,)), dma((fsdp,)),
            ]

        def grant(mebibytes, ident=None):
            if ident is None:
                return pltpu.CompilerParams(vmem_limit_bytes=mebibytes * 2**20)
            return pltpu.CompilerParams(
                collective_id=ident, has_side_effects=True, vmem_limit_bytes=mebibytes * 2**20)

        whole = jax.ShapeDtypeStruct((chunks, rows, fsdp * width), jnp.bfloat16)
        master = master.reshape(experts, fsdp, own, width)
        second = second.reshape(experts, fsdp, own, width)
        most, first = max(cuts), 3 * AHEAD
        early, scales, routers = pl.pallas_call(
            functools.partial(exchange, dims, [(0, cut) for cut in cuts], first),
            out_shape=(
                pltpu.VMEM((most, rows, fsdp * width), jnp.bfloat16),
                pltpu.VMEM((most, 1, LANES), jnp.float32),
                pltpu.VMEM((groups, fsdp, columns, width), jnp.bfloat16),
            ),
            in_specs=[hbm, hbm, hbm, hbm],
            out_specs=(inside, inside, inside),
            scratch_shapes=[
                pltpu.VMEM((columns, width), jnp.float32),
                pltpu.VMEM((1, width), jnp.float32),
                pltpu.VMEM((columns, width), jnp.bfloat16),
                pltpu.VMEM((first, fsdp, half, 2, LANES), jnp.float32),
                dma((2,)), dma((first,)), dma((first,)), dma((2,)), dma((2,)),
            ] + scratch(most),
            compiler_params=grant(28, 0),
            name="exchange_early",
        )(
            master,
            second,
            pltpu.with_memory_space_constraint(router.T, pltpu.HBM),
            pltpu.with_memory_space_constraint(gain[None, :], pltpu.HBM),
        )
        final, router = pl.pallas_call(
            functools.partial(write_first, cuts, steps),
            out_shape=(whole, jax.ShapeDtypeStruct((groups * columns, fsdp * width), jnp.bfloat16)),
            in_specs=[inside, inside],
            out_specs=(hbm, hbm),
            scratch_shapes=[
                pltpu.VMEM((groups * columns, fsdp * width), jnp.bfloat16),
                dma((experts + 2,)),
            ],
            compiler_params=grant(2),
            name="write_early",
        )(early, routers)
        most = chunks - min(cuts)
        late, late_scales = pl.pallas_call(
            functools.partial(exchange, dims, [(cut, chunks) for cut in cuts], 0),
            out_shape=(
                pltpu.VMEM((most, rows, fsdp * width), jnp.bfloat16),
                pltpu.VMEM((most, 1, LANES), jnp.float32),
            ),
            in_specs=[hbm, hbm, hbm],
            out_specs=(inside, inside),
            scratch_shapes=scratch(most),
            compiler_params=grant(28, 1),
            name="exchange_late",
        )(master, second, pltpu.with_memory_space_constraint(router, pltpu.HBM))
        final, scale = pl.pallas_call(
            functools.partial(write_second, cuts, chunks, steps),
            out_shape=(whole, jax.ShapeDtypeStruct((experts, own), jnp.float32)),
            in_specs=[hbm, inside, inside, inside],
            out_specs=(hbm, hbm),
            scratch_shapes=[pltpu.VMEM((experts, own), jnp.float32), dma((2,))],
            input_output_aliases={0: 0},
            compiler_params=grant(2),
            name="write_late",
        )(final, late, scales, late_scales)
        return final.reshape(experts, own, fsdp * width), scale, router.T

    return jax.shard_map(
        step,
        mesh=mesh,
        in_specs=(P("ep", None, "fsdp"), P("ep", None, "fsdp"), P("fsdp", "ep"), P("fsdp")),
        out_specs=(P("ep", "fsdp", None), P("ep", "fsdp"), P()),
        check_vma=False,
    )
```
